32 devices in a mesh: dp: 16 (over z, y, x), mp: 2 (over core).
Axes of the slice: x: 2, y: 2, z: 4, core: 2. Of those that a mesh axis runs over, the one named last changes fastest.
Arguments:
- pre_act: bfloat16 [8192, 16384], P('dp', 'mp'), may hold values from -8 to 8
- out_weight: bfloat16 [16384, 512], P('mp'), may hold values from -0.046875 to 0.046875
- out_grad: bfloat16 [8192, 512], P(('dp', 'mp')), may hold values from -2 to 2
Outputs:
- projected: bfloat16 [8192, 512], P(('dp', 'mp'))
- combined: float32 [16384, 512], P(('mp', 'dp'))
The draws below stay inside these ranges and needn't reach their ends.
All inputs are finite; a program needn't handle non-finite values.
Results may differ from the reference program's by a relative error of at most 0.0005.
Values may be sent and summed in bfloat16 or wider, within the bound.
A program may use at most 128 MiB of HBM per device.

```python
import math
import jax
import jax.numpy as jnp
from jax import lax

D = 512
FF = 16384
TOK_DEV = 512
TOKENS = 8192
N_DP = 16


def draw_pre_act(key, part):
    base = jax.random.normal(jax.random.fold_in(key, 11), (FF,), jnp.float32)
    noise = jax.random.normal(jax.random.fold_in(key, 12), (TOKENS, FF), jnp.float32)
    values = 0.6 * base[None, :] + noise
    return jnp.clip(values, -8.0, 8.0).astype(jnp.bfloat16)


def draw_out_grad(key, part):
    base = jax.random.normal(jax.random.fold_in(key, 21), (D,), jnp.float32)
    block_count = TOKENS // TOK_DEV
    block_scale = jnp.exp(jax.random.uniform(jax.random.fold_in(key, 23), (block_count,), jnp.float32, 0.0, math.log(10.0)))
    row_scale = jnp.exp(jax.random.uniform(jax.random.fold_in(key, 24), (TOKENS,), jnp.float32, -0.5, 0.5))
    scales = jnp.repeat(block_scale, TOK_DEV) * row_scale
    noise = jax.random.normal(jax.random.fold_in(key, 22), (TOKENS, D), jnp.float32)
    values = 0.06 * base[None, :] + noise
    return jnp.clip(0.025 * scales[:, None] * values, -2.0, 2.0).astype(jnp.bfloat16)


def levels(own_key, dims, split, low, top_value):
    gain, own = 1.0, jax.random.fold_in(own_key, 6)
    for axis_at, shards_of in split:
        draws = jnp.exp(jax.random.uniform(jax.random.fold_in(own, axis_at), (shards_of,), jnp.float32, low / len(split), top_value / len(split)))
        gain = gain * jnp.repeat(draws, dims[axis_at] // shards_of).reshape([-1 if axis == axis_at else 1 for axis in range(len(dims))])
    return gain


def scatter_about(key, shape, spread, reach, shards=(), held_as=jnp.bfloat16):
    entries = jax.random.normal(key, shape, jnp.float32) * spread
    if len(shards) > 0:
        entries = levels(key, shape, shards, -0.22, 0.18) * entries
    return jnp.clip(entries, min=-reach, max=reach).astype(held_as)


def setup_inputs(seed: int = 0) -> dict:
    key_of = jax.random.split(jax.random.key(seed), 4)
    return {
        "pre_act": draw_pre_act(jax.random.fold_in(key_of[3], 71), 0),
        "out_weight": scatter_about(key_of[1], (FF, D), FF ** -0.5, 0.046875, ((0, 2),)),
        "out_grad": draw_out_grad(jax.random.fold_in(key_of[3], 71), 0),
    }


epsilon = 1e-6


def pair(first, second):
    inner = jnp.sum(first * second)
    first_sq = jnp.sum(first * first)
    second_sq = jnp.sum(second * second)
    return (1.0 - inner / (2.0 * (first_sq + epsilon))) * first + (1.0 - inner / (2.0 * (second_sq + epsilon))) * second


def reference(pre_act, out_weight, out_grad):
    act = jnp.maximum(pre_act, jnp.zeros((), jnp.bfloat16))
    projected = jnp.dot(act, out_weight, preferred_element_type=jnp.float32).astype(jnp.bfloat16)

    def leaf(index):
        rows = act[index * TOK_DEV:(index + 1) * TOK_DEV]
        grads = out_grad[index * TOK_DEV:(index + 1) * TOK_DEV]
        return lax.dot_general(rows, grads, (((0,), (0,)), ((), ())), preferred_element_type=jnp.float32)

    def build(low, count):
        if count == 1:
            return leaf(low)
        half = count // 2
        return pair(build(low, half), build(low + half, half))

    combined = build(0, N_DP)
    return projected, combined
```

```python
import functools
import jax
import jax.numpy as jnp
from jax import lax
from jax.experimental import pallas as pl
from jax.experimental.pallas import tpu as pltpu
from jax.sharding import PartitionSpec as P

epsilon = 1e-06
MESH = pl.DeviceIdType.MESH


def from_partner(value, axis, apart):
    mask = 2**apart
    pairs = [(source, source ^ mask) for source in range(lax.axis_size(axis))]
    return lax.ppermute(value, axis, pairs)


def contract(left, right):
    return lax.dot_general(
        left, right, (((0,), (0,)), ((), ())), preferred_element_type=jnp.float32
    )


def split_rows(piece, block, which):
    width = piece.shape[1]
    blocks = piece.reshape(piece.shape[0] // (2 * block), 2, block, width)
    kept = lax.dynamic_index_in_dim(blocks, which, 1, False).reshape(-1, width)
    sent = lax.dynamic_index_in_dim(blocks, 1 - which, 1, False).reshape(-1, width)
    return (kept, sent)


def level_sums(partial_value, level):
    totals = lax.psum(partial_value, "mp")
    for inner_bit in range(level + 1):
        totals = totals + from_partner(totals, "dp", inner_bit)
    return totals


def merge_level(own, other, level, which):
    lower = which == 0
    own_sq = jnp.sum(own * own)
    other_sq = jnp.sum(other * other)
    partial_value = jnp.stack(
        [
            jnp.sum(own * other),
            jnp.where(lower, own_sq, other_sq),
            jnp.where(lower, other_sq, own_sq),
        ]
    )
    totals = level_sums(partial_value, level)
    first_coef = 1.0 - totals[0] / (2.0 * (totals[1] + epsilon))
    second_coef = 1.0 - totals[0] / (2.0 * (totals[2] + epsilon))
    own_coef = jnp.where(lower, first_coef, second_coef)
    other_coef = jnp.where(lower, second_coef, first_coef)
    return own_coef * own + other_coef * other


def halving(pre_act, out_weight, out_grad):
    act = jnp.maximum(pre_act, jnp.zeros((), jnp.bfloat16))
    tokens = act.shape[0]
    partial_out = jnp.dot(act, out_weight, preferred_element_type=jnp.float32)
    summed = lax.psum_scatter(partial_out, "mp", scatter_dimension=0, tiled=True)
    projected = summed.astype(jnp.bfloat16)
    grad_full = lax.all_gather(out_grad, "mp", axis=0, tiled=True)
    count = lax.axis_size("dp")
    levels = count.bit_length() - 1
    me = lax.axis_index("dp")
    block = act.shape[1] // count
    first_bit = me & 1
    groups = act.reshape(tokens, act.shape[1] // (2 * block), 2, block)
    kept_act = lax.dynamic_index_in_dim(groups, first_bit, 2, False).reshape(tokens, -1)
    sent_act = lax.dynamic_index_in_dim(groups, 1 - first_bit, 2, False).reshape(tokens, -1)
    packed = jnp.concatenate([sent_act, grad_full], axis=1)
    arrived = from_partner(packed, "dp", 0)
    half = sent_act.shape[1]
    own = contract(kept_act, grad_full)
    other = contract(arrived[:, :half], arrived[:, half:])
    piece = merge_level(own, other, 0, first_bit)
    for level in range(1, levels):
        which = me >> level & 1
        own, sent = split_rows(piece, block, which)
        other = from_partner(sent, "dp", level)
        piece = merge_level(own, other, level, which)
    return (projected, piece)


def put_lanes(values, rows):
    padded = -(-len(values) // 8) * 8
    strips = [jnp.sum(v, axis=0, keepdims=True) for v in values]
    strips += [jnp.zeros_like(strips[0])] * (padded - len(values))
    table = jnp.concatenate(strips, axis=0)
    totals = jnp.sum(table, axis=1, keepdims=True)
    lane = lax.broadcasted_iota(jnp.int32, table.shape, 1)
    row = lax.broadcasted_iota(jnp.int32, table.shape, 0)
    line = jnp.sum(jnp.where(lane == row, totals, 0.0), axis=0, keepdims=True)
    return jnp.broadcast_to(line, (rows, line.shape[1]))


def lane_value(line, p):
    lane = lax.broadcasted_iota(jnp.int32, line.shape, 1)
    return jnp.sum(jnp.where(lane == p, line, 0.0), axis=1, keepdims=True)


def kernel(
    n_dp, pre, w, og, proj, comb,
    acts, grads_in, leaf, node, arrived, xbuf, wbuf, acc, part_in, slots, slots3,
    act_send, act_recv, og_send, og_recv, mate_send, mate_recv, local_sem, own_sem,
    fwd_sem, part_sem, slot_send, slot_recv, node_send, node_recv, slot3_send, slot3_recv,
):
    dp = lax.axis_index("dp")
    core = lax.axis_index("mp")
    group = n_dp // 2
    bits = group.bit_length() - 1
    me = lax.rem(dp, group)
    high = dp // group
    base = high * group
    tokens = pre.shape[0]
    block = pre.shape[1] // n_dp
    own_rows = og.shape[0]
    width = og.shape[1]
    mate = 1 - core
    me_bits = [lax.rem(me // 2**b, 2) for b in range(bits)]

    def flip(r):
        total = 0
        for b in range(bits):
            rb = (r // 2**b) % 2 if isinstance(r, int) else lax.rem(r // 2**b, 2)
            total = total + 2**b * (me_bits[b] + rb - 2 * me_bits[b] * rb)
        return total

    barrier = pltpu.get_barrier_semaphore()
    for q in range(1, 2 * n_dp):
        other = lax.rem(dp * 2 + core + q, 2 * n_dp)
        pl.semaphore_signal(
            barrier, inc=1, device_id=(other // 2, lax.rem(other, 2)), device_id_type=MESH
        )

    my_og = grads_in.at[me, pl.ds(core * own_rows, own_rows)]
    og_local = pltpu.make_async_copy(og, my_og, local_sem)
    og_local.start()

    def own_copy(h):
        cols = pl.ds(pl.multiple_of((me + group * h) * block, block), block)
        return pltpu.make_async_copy(pre.at[:, cols], acts.at[me, h], own_sem.at[h])

    own_copy(0).start()
    own_copy(1).start()
    og_local.wait()
    pl.semaphore_wait(barrier, 2 * n_dp - 1)

    def og_copy(r, i, at):
        rows = grads_in.at[at, pl.ds(core * own_rows, own_rows)]
        return pltpu.make_async_remote_copy(
            src_ref=rows, dst_ref=rows, send_sem=og_send.at[r], recv_sem=og_recv.at[r],
            device_id=(base + i, core), device_id_type=MESH,
        )

    def act_copy(r, i, h, at):
        cols = pl.ds(pl.multiple_of((i + group * h) * block, block), block)
        return pltpu.make_async_remote_copy(
            src_ref=pre.at[:, cols], dst_ref=acts.at[at, h],
            send_sem=act_send.at[r, h], recv_sem=act_recv.at[r, h],
            device_id=(base + i, core), device_id_type=MESH,
        )

    def mate_copy(r, i, side):
        rows = grads_in.at[i, pl.ds(side * own_rows, own_rows)]
        return pltpu.make_async_remote_copy(
            src_ref=rows, dst_ref=rows, send_sem=mate_send.at[r], recv_sem=mate_recv.at[r],
            device_id=(dp, mate), device_id_type=MESH,
        )

    mate_copy(0, me, core).start()
    order = ORDER if group == 8 else list(range(1, group))
    for r in order:
        og_copy(r, flip(r), me).start()
    for h in range(2):
        for r in order:
            act_copy(r, flip(r), h, me).start()

    step_cols = xbuf.shape[2]
    steps = pre.shape[1] // step_cols

    def fetch(k, slot):
        cols = pl.ds(pl.multiple_of(k * step_cols, step_cols), step_cols)
        return (
            pltpu.make_async_copy(pre.at[:, cols], xbuf.at[slot], fwd_sem.at[slot, 0]),
            pltpu.make_async_copy(w.at[cols, :], wbuf.at[slot], fwd_sem.at[slot, 1]),
        )

    for c in fetch(0, 0):
        c.start()
    acc[...] = jnp.zeros_like(acc)

    def forward(k, carry):
        slot = lax.rem(k, 2)

        @pl.when(k + 1 < steps)
        def _():
            for c in fetch(k + 1, 1 - slot):
                c.start()

        for c in fetch(k, slot):
            c.wait()
        x = jnp.maximum(xbuf[slot], jnp.zeros((), jnp.bfloat16))
        acc[...] += jnp.dot(x, wbuf[slot], preferred_element_type=jnp.float32)
        return carry

    lax.fori_loop(0, steps, forward, 0)
    part = pltpu.make_async_remote_copy(
        src_ref=acc.at[pl.ds(mate * own_rows, own_rows)], dst_ref=part_in,
        send_sem=part_sem.at[0], recv_sem=part_sem.at[1],
        device_id=(dp, mate), device_id_type=MESH,
    )
    part.start()

    for r in order:
        i = flip(r)
        og_copy(r, i, i).wait_recv()
        mate_copy(r, i, core).start()
    part.wait_recv()
    proj[...] = (acc[pl.ds(core * own_rows, own_rows), :] + part_in[...]).astype(proj.dtype)
    for r in range(group):
        mate_copy(r, flip(r), mate).wait_recv()

    pairs = [(i, j) for i in range(group) for j in range(i, group)]
    sums = tuple(jnp.zeros((8, 128), jnp.float32) for _ in pairs)
    for h in range(2):
        def leaf_grad(i):
            a = jnp.maximum(acts[i, h], jnp.zeros((), jnp.bfloat16))
            leaf[i, pl.ds(h * block, block), :] = contract(a, grads_in[i])

        own_copy(h).wait()
        leaf_grad(me)
        for r in order:
            i = flip(r)
            act_copy(r, i, h, i).wait_recv()
            leaf_grad(i)

        def gram(t, carry):
            rows = pl.ds(pl.multiple_of(h * block + t * 8, 8), 8)
            for c in range(width // 128):
                v = [leaf[i, rows, c * 128:(c + 1) * 128] for i in range(group)]
                carry = tuple(s + v[i] * v[j] for s, (i, j) in zip(carry, pairs))
            return carry

        sums = lax.fori_loop(0, block // 8, gram, sums)

    mine = me * 2 + core
    slots[mine] = put_lanes(list(sums), 8)

    def slot_copy(q, other, at):
        return pltpu.make_async_remote_copy(
            src_ref=slots.at[at], dst_ref=slots.at[at],
            send_sem=slot_send.at[q], recv_sem=slot_recv.at[at],
            device_id=(base + other // 2, lax.rem(other, 2)), device_id_type=MESH,
        )

    for q in range(1, 2 * group):
        slot_copy(q, lax.rem(mine + q, 2 * group), mine).start()
    for q in range(1, 2 * group):
        other = lax.rem(mine + q, 2 * group)
        slot_copy(q, other, other).wait_recv()
    line = slots[0]
    for k in range(1, 2 * group):
        line = line + slots[k]
    line = line[0:1]
    table = {}
    for p, (i, j) in enumerate(pairs):
        table[i, j] = table[j, i] = lane_value(line, p)
    coef = [jnp.ones((1, 1), jnp.float32) for _ in range(group)]

    def form(left, right):
        total = jnp.zeros((1, 1), jnp.float32)
        for i in left:
            for j in right:
                total = total + coef[i] * coef[j] * table[i, j]
        return total

    for level in range(bits):
        size = 2**level
        fresh = list(coef)
        for start in range(0, group, 2 * size):
            left = range(start, start + size)
            right = range(start + size, start + 2 * size)
            s = form(left, right)
            first = 1.0 - s / (2.0 * (jnp.maximum(form(left, left), 0.0) + epsilon))
            second = 1.0 - s / (2.0 * (jnp.maximum(form(right, right), 0.0) + epsilon))
            for i in left:
                fresh[i] = coef[i] * first
            for j in right:
                fresh[j] = coef[j] * second
        coef = fresh

    wide = [jnp.broadcast_to(c, (8, width)) for c in coef]

    def build(h):
        def strip(t, carry):
            rows = pl.ds(pl.multiple_of(h * block + t * 8, 8), 8)
            total = wide[0] * leaf[0, rows, :]
            for i in range(1, group):
                total = total + wide[i] * leaf[i, rows, :]
            node[h, pl.ds(pl.multiple_of(t * 8, 8), 8), :] = total
            return carry
        lax.fori_loop(0, block // 8, strip, 0)

    far = lax.rem(dp + group, n_dp)
    pieces = node_send.shape[0]
    tall = block // pieces

    def node_copy(k):
        rows = pl.ds(k * tall, tall)
        return pltpu.make_async_remote_copy(
            src_ref=node.at[1 - high, rows], dst_ref=arrived.at[rows],
            send_sem=node_send.at[k], recv_sem=node_recv.at[k],
            device_id=(far, core), device_id_type=MESH,
        )

    build(1 - high)
    for k in range(pieces):
        node_copy(k).start()
    build(high)

    sums = tuple(jnp.zeros((8, 128), jnp.float32) for _ in range(3))
    for k in range(pieces):
        node_copy(k).wait_recv()

        def inner(t, carry):
            rows = pl.ds(pl.multiple_of(k * tall + t * 8, 8), 8)
            s, q, r = carry
            for c in range(width // 128):
                a = node[high, rows, c * 128:(c + 1) * 128]
                b = arrived[rows, c * 128:(c + 1) * 128]
                s, q, r = s + a * b, q + a * a, r + b * b
            return s, q, r

        sums = lax.fori_loop(0, tall // 8, inner, sums)
    up = high.astype(jnp.float32)
    low_sq = (1.0 - up) * sums[1] + up * sums[2]
    high_sq = up * sums[1] + (1.0 - up) * sums[2]
    place = dp * 2 + core
    slots3[place] = put_lanes([sums[0], low_sq, high_sq], 8)

    def slot3_copy(q, other, at):
        return pltpu.make_async_remote_copy(
            src_ref=slots3.at[at], dst_ref=slots3.at[at],
            send_sem=slot3_send.at[q], recv_sem=slot3_recv.at[at],
            device_id=(other // 2, lax.rem(other, 2)), device_id_type=MESH,
        )

    for q in range(1, 2 * n_dp):
        slot3_copy(q, lax.rem(place + q, 2 * n_dp), place).start()
    for q in range(1, 2 * n_dp):
        other = lax.rem(place + q, 2 * n_dp)
        slot3_copy(q, other, other).wait_recv()
    line = slots3[0]
    for k in range(1, 2 * n_dp):
        line = line + slots3[k]
    line = line[0:1]
    s = lane_value(line, 0)
    low = 1.0 - s / (2.0 * (lane_value(line, 1) + epsilon))
    top = 1.0 - s / (2.0 * (lane_value(line, 2) + epsilon))
    own_coef = jnp.broadcast_to((1.0 - up) * low + up * top, (8, width))
    far_coef = jnp.broadcast_to(up * low + (1.0 - up) * top, (8, width))

    def last(t, carry):
        rows = pl.ds(pl.multiple_of(t * 8, 8), 8)
        comb[rows, :] = own_coef * node[high, rows, :] + far_coef * arrived[rows, :]
        return carry

    lax.fori_loop(0, block // 8, last, 0)

    mate_copy(0, me, core).wait_send()
    for r in order:
        i = flip(r)
        og_copy(r, i, me).wait_send()
        mate_copy(r, i, core).wait_send()
        for h in range(2):
            act_copy(r, i, h, me).wait_send()
    part.wait_send()
    for q in range(1, 2 * group):
        slot_copy(q, lax.rem(mine + q, 2 * group), mine).wait_send()
    for k in range(pieces):
        node_copy(k).wait_send()
    for q in range(1, 2 * n_dp):
        slot3_copy(q, lax.rem(place + q, 2 * n_dp), place).wait_send()


ORDER = [7, 3, 5, 6, 1, 2, 4]


def exchange(n_dp, pre_act, out_weight, out_grad):
    tokens, hidden = pre_act.shape
    block = hidden // n_dp
    group = n_dp // 2
    width = out_grad.shape[1]
    own_rows = out_grad.shape[0]
    step_cols = hidden // 8
    pieces = 4
    dma = pltpu.SemaphoreType.DMA
    hbm = pl.BlockSpec(memory_space=pl.ANY)
    vmem = pl.BlockSpec(memory_space=pltpu.VMEM)
    return pl.pallas_call(
        functools.partial(kernel, n_dp),
        out_shape=(
            jax.ShapeDtypeStruct((own_rows, width), jnp.bfloat16),
            jax.ShapeDtypeStruct((block, width), jnp.float32),
        ),
        in_specs=[hbm, hbm, hbm],
        out_specs=(vmem, vmem),
        scratch_shapes=[
            pltpu.VMEM((group, 2, tokens, block), jnp.bfloat16),
            pltpu.VMEM((group, tokens, width), jnp.bfloat16),
            pltpu.VMEM((group, 2 * block, width), jnp.float32),
            pltpu.VMEM((2, block, width), jnp.float32),
            pltpu.VMEM((block, width), jnp.float32),
            pltpu.VMEM((2, tokens, step_cols), jnp.bfloat16),
            pltpu.VMEM((2, step_cols, width), jnp.bfloat16),
            pltpu.VMEM((tokens, width), jnp.float32),
            pltpu.VMEM((own_rows, width), jnp.float32),
            pltpu.VMEM((2 * group, 8, 128), jnp.float32),
            pltpu.VMEM((2 * n_dp, 8, 128), jnp.float32),
            dma((group, 2)), dma((group, 2)), dma((group,)), dma((group,)),
            dma((group,)), dma((group,)), dma, dma((2,)),
            dma((2, 2)), dma((2,)), dma((2 * group,)), dma((2 * group,)),
            dma((pieces,)), dma((pieces,)), dma((2 * n_dp,)), dma((2 * n_dp,)),
        ],
        compiler_params=pltpu.CompilerParams(
            collective_id=0, has_side_effects=True, vmem_limit_bytes=60 * 2**20
        ),
    )(pre_act, out_weight, out_grad)


def local(pre_act, out_weight, out_grad):
    n_dp = lax.axis_size("dp")
    block = pre_act.shape[1] // n_dp
    rows = out_grad.shape[0]
    if lax.axis_size("mp") == 2 and n_dp <= 16 and block % 128 == 0 and rows % 16 == 0:
        return exchange(n_dp, pre_act, out_weight, out_grad)
    return halving(pre_act, out_weight, out_grad)


def solution(mesh):
    placed = (P("dp", "mp"), P("mp", None), P(("dp", "mp"), None))
    return jax.shard_map(
        local,
        mesh=mesh,
        in_specs=placed,
        out_specs=(P(("dp", "mp"), None), P(("mp", "dp"), None)),
        check_vma=False,
    )
```

```python
import functools
import jax
import jax.numpy as jnp
from jax import lax
from jax.experimental import pallas as pl
from jax.experimental.pallas import tpu as pltpu
from jax.sharding import PartitionSpec as P

epsilon = 1e-06
MESH = pl.DeviceIdType.MESH


def from_partner(value, axis, apart):
    mask = 2**apart
    pairs = [(source, source ^ mask) for source in range(lax.axis_size(axis))]
    return lax.ppermute(value, axis, pairs)


def contract(left, right):
    return lax.dot_general(
        left, right, (((0,), (0,)), ((), ())), preferred_element_type=jnp.float32
    )


def split_rows(piece, block, which):
    width = piece.shape[1]
    blocks = piece.reshape(piece.shape[0] // (2 * block), 2, block, width)
    kept = lax.dynamic_index_in_dim(blocks, which, 1, False).reshape(-1, width)
    sent = lax.dynamic_index_in_dim(blocks, 1 - which, 1, False).reshape(-1, width)
    return (kept, sent)


def level_sums(partial_value, level):
    totals = lax.psum(partial_value, "mp")
    for inner_bit in range(level + 1):
        totals = totals + from_partner(totals, "dp", inner_bit)
    return totals


def merge_level(own, other, level, which):
    lower = which == 0
    own_sq = jnp.sum(own * own)
    other_sq = jnp.sum(other * other)
    partial_value = jnp.stack(
        [
            jnp.sum(own * other),
            jnp.where(lower, own_sq, other_sq),
            jnp.where(lower, other_sq, own_sq),
        ]
    )
    totals = level_sums(partial_value, level)
    first_coef = 1.0 - totals[0] / (2.0 * (totals[1] + epsilon))
    second_coef = 1.0 - totals[0] / (2.0 * (totals[2] + epsilon))
    own_coef = jnp.where(lower, first_coef, second_coef)
    other_coef = jnp.where(lower, second_coef, first_coef)
    return own_coef * own + other_coef * other


def halving(pre_act, out_weight, out_grad):
    act = jnp.maximum(pre_act, jnp.zeros((), jnp.bfloat16))
    tokens = act.shape[0]
    partial_out = jnp.dot(act, out_weight, preferred_element_type=jnp.float32)
    summed = lax.psum_scatter(partial_out, "mp", scatter_dimension=0, tiled=True)
    projected = summed.astype(jnp.bfloat16)
    grad_full = lax.all_gather(out_grad, "mp", axis=0, tiled=True)
    count = lax.axis_size("dp")
    levels = count.bit_length() - 1
    me = lax.axis_index("dp")
    block = act.shape[1] // count
    first_bit = me & 1
    groups = act.reshape(tokens, act.shape[1] // (2 * block), 2, block)
    kept_act = lax.dynamic_index_in_dim(groups, first_bit, 2, False).reshape(tokens, -1)
    sent_act = lax.dynamic_index_in_dim(groups, 1 - first_bit, 2, False).reshape(tokens, -1)
    packed = jnp.concatenate([sent_act, grad_full], axis=1)
    arrived = from_partner(packed, "dp", 0)
    half = sent_act.shape[1]
    own = contract(kept_act, grad_full)
    other = contract(arrived[:, :half], arrived[:, half:])
    piece = merge_level(own, other, 0, first_bit)
    for level in range(1, levels):
        which = me >> level & 1
        own, sent = split_rows(piece, block, which)
        other = from_partner(sent, "dp", level)
        piece = merge_level(own, other, level, which)
    return (projected, piece)


def put_lanes(values, rows):
    padded = -(-len(values) // 8) * 8
    strips = [jnp.sum(v, axis=0, keepdims=True) for v in values]
    strips += [jnp.zeros_like(strips[0])] * (padded - len(values))
    table = jnp.concatenate(strips, axis=0)
    totals = jnp.sum(table, axis=1, keepdims=True)
    lane = lax.broadcasted_iota(jnp.int32, table.shape, 1)
    row = lax.broadcasted_iota(jnp.int32, table.shape, 0)
    line = jnp.sum(jnp.where(lane == row, totals, 0.0), axis=0, keepdims=True)
    return jnp.broadcast_to(line, (rows, line.shape[1]))


def lane_value(line, p):
    lane = lax.broadcasted_iota(jnp.int32, line.shape, 1)
    return jnp.sum(jnp.where(lane == p, line, 0.0), axis=1, keepdims=True)


def kernel(
    n_dp, pre, w, og, proj, comb,
    acts, grads_in, leaf, node, arrived, xbuf, wbuf, acc, part_in, slots, slots3,
    act_send, act_recv, og_send, og_recv, mate_send, mate_recv, local_sem, own_sem,
    fwd_sem, part_sem, slot_send, slot_recv, node_send, node_recv, slot3_send, slot3_recv,
):
    dp = lax.axis_index("dp")
    core = lax.axis_index("mp")
    group = n_dp // 2
    bits = group.bit_length() - 1
    me = lax.rem(dp, group)
    high = dp // group
    base = high * group
    tokens = pre.shape[0]
    block = pre.shape[1] // n_dp
    own_rows = og.shape[0]
    width = og.shape[1]
    mate = 1 - core
    me_bits = [lax.rem(me // 2**b, 2) for b in range(bits)]

    def flip(r):
        total = 0
        for b in range(bits):
            rb = (r // 2**b) % 2 if isinstance(r, int) else lax.rem(r // 2**b, 2)
            total = total + 2**b * (me_bits[b] + rb - 2 * me_bits[b] * rb)
        return total

    barrier = pltpu.get_barrier_semaphore()
    for q in range(1, 2 * n_dp):
        other = lax.rem(dp * 2 + core + q, 2 * n_dp)
        pl.semaphore_signal(
            barrier, inc=1, device_id=(other // 2, lax.rem(other, 2)), device_id_type=MESH
        )

    my_og = grads_in.at[me, pl.ds(core * own_rows, own_rows)]
    og_local = pltpu.make_async_copy(og, my_og, local_sem)
    og_local.start()

    def own_copy(h):
        cols = pl.ds(pl.multiple_of((me + group * h) * block, block), block)
        return pltpu.make_async_copy(pre.at[:, cols], acts.at[me, h], own_sem.at[h])

    own_copy(0).start()
    own_copy(1).start()
    og_local.wait()
    pl.semaphore_wait(barrier, 2 * n_dp - 1)

    def og_copy(r):
        at, to = flip(RELAY[r][0]), flip(RELAY[r][1])
        rows = grads_in.at[at, pl.ds(core * own_rows, own_rows)]
        return pltpu.make_async_remote_copy(
            src_ref=rows, dst_ref=rows, send_sem=og_send.at[r], recv_sem=og_recv.at[r],
            device_id=(base + to, core), device_id_type=MESH,
        )

    def og_arrival(r):
        rows = grads_in.at[flip(r), pl.ds(core * own_rows, own_rows)]
        pltpu.make_async_remote_copy(
            src_ref=rows, dst_ref=rows, send_sem=og_send.at[r], recv_sem=og_recv.at[r],
            device_id=(base + flip(r), core), device_id_type=MESH,
        ).wait_recv()
        mate_copy(r, flip(r), core).start()

    def act_copy(r, i, h, at):
        cols = pl.ds(pl.multiple_of((i + group * h) * block, block), block)
        return pltpu.make_async_remote_copy(
            src_ref=pre.at[:, cols], dst_ref=acts.at[at, h],
            send_sem=act_send.at[r, h], recv_sem=act_recv.at[r, h],
            device_id=(base + i, core), device_id_type=MESH,
        )

    def mate_copy(r, i, side):
        rows = grads_in.at[i, pl.ds(side * own_rows, own_rows)]
        return pltpu.make_async_remote_copy(
            src_ref=rows, dst_ref=rows, send_sem=mate_send.at[r], recv_sem=mate_recv.at[r],
            device_id=(dp, mate), device_id_type=MESH,
        )

    mate_copy(0, me, core).start()
    for r in (4, 1, 2):
        og_copy(r).start()
    act_copy(7, flip(7), 0, me).start()
    og_arrival(2)
    og_copy(6).start()
    for h in range(2):
        for lead, _ in SLOTS:
            if (lead, h) != (7, 0):
                act_copy(lead, flip(lead), h, me).start()
    og_arrival(4)
    og_copy(5).start()
    og_arrival(1)
    og_copy(3).start()
    for h in range(2):
        for r in (2, 1, 3):
            act_copy(r, flip(r), h, me).start()

    step_cols = xbuf.shape[2]
    steps = pre.shape[1] // step_cols

    def fetch(k, slot):
        cols = pl.ds(pl.multiple_of(k * step_cols, step_cols), step_cols)
        return (
            pltpu.make_async_copy(pre.at[:, cols], xbuf.at[slot], fwd_sem.at[slot, 0]),
            pltpu.make_async_copy(w.at[cols, :], wbuf.at[slot], fwd_sem.at[slot, 1]),
        )

    for c in fetch(0, 0):
        c.start()
    acc[...] = jnp.zeros_like(acc)

    def forward(k, carry):
        slot = lax.rem(k, 2)

        @pl.when(k + 1 < steps)
        def _():
            for c in fetch(k + 1, 1 - slot):
                c.start()

        for c in fetch(k, slot):
            c.wait()
        x = jnp.maximum(xbuf[slot], jnp.zeros((), jnp.bfloat16))
        acc[...] += jnp.dot(x, wbuf[slot], preferred_element_type=jnp.float32)
        return carry

    lax.fori_loop(0, steps, forward, 0)
    part = pltpu.make_async_remote_copy(
        src_ref=acc.at[pl.ds(mate * own_rows, own_rows)], dst_ref=part_in,
        send_sem=part_sem.at[0], recv_sem=part_sem.at[1],
        device_id=(dp, mate), device_id_type=MESH,
    )
    part.start()

    og_arrival(6)
    og_copy(7).start()
    for r in (5, 3, 7):
        og_arrival(r)
    part.wait_recv()
    proj[...] = (acc[pl.ds(core * own_rows, own_rows), :] + part_in[...]).astype(proj.dtype)
    for r in range(group):
        mate_copy(r, flip(r), mate).wait_recv()

    pairs = [(i, j) for i in range(group) for j in range(i, group)]
    sums = tuple(jnp.zeros((8, 128), jnp.float32) for _ in pairs)
    def gram_rows(h, sums):
        def gram(t, carry):
            rows = pl.ds(pl.multiple_of(h * block + t * 8, 8), 8)
            for c in range(width // 128):
                v = [leaf[i, rows, c * 128:(c + 1) * 128] for i in range(group)]
                carry = tuple(s + v[i] * v[j] for s, (i, j) in zip(carry, pairs))
            return carry

        return lax.fori_loop(0, block // 8, gram, sums)

    for h in range(2):
        def leaf_grad(i):
            a = jnp.maximum(acts[i, h], jnp.zeros((), jnp.bfloat16))
            leaf[i, pl.ds(h * block, block), :] = contract(a, grads_in[i])

        own_copy(h).wait()
        leaf_grad(me)
        for n, (lead, beside) in enumerate(SLOTS):
            act_copy(lead, flip(lead), h, me).wait_send()
            if h == 1 and n == 0:
                sums = gram_rows(0, sums)
            for r in (lead, beside):
                if r:
                    i = flip(r)
                    act_copy(r, i, h, i).wait_recv()
                    leaf_grad(i)

        if h == 1:
            sums = gram_rows(1, sums)

    mine = me * 2 + core
    slots[mine] = put_lanes(list(sums), 8)

    def slot_copy(q, other, at):
        return pltpu.make_async_remote_copy(
            src_ref=slots.at[at], dst_ref=slots.at[at],
            send_sem=slot_send.at[q], recv_sem=slot_recv.at[at],
            device_id=(base + other // 2, lax.rem(other, 2)), device_id_type=MESH,
        )

    for q in range(1, 2 * group):
        slot_copy(q, lax.rem(mine + q, 2 * group), mine).start()
    for q in range(1, 2 * group):
        other = lax.rem(mine + q, 2 * group)
        slot_copy(q, other, other).wait_recv()
    line = slots[0]
    for k in range(1, 2 * group):
        line = line + slots[k]
    line = line[0:1]
    table = {}
    for p, (i, j) in enumerate(pairs):
        table[i, j] = table[j, i] = lane_value(line, p)
    coef = [jnp.ones((1, 1), jnp.float32) for _ in range(group)]

    def form(left, right):
        total = jnp.zeros((1, 1), jnp.float32)
        for i in left:
            for j in right:
                total = total + coef[i] * coef[j] * table[i, j]
        return total

    for level in range(bits):
        size = 2**level
        fresh = list(coef)
        for start in range(0, group, 2 * size):
            left = range(start, start + size)
            right = range(start + size, start + 2 * size)
            s = form(left, right)
            first = 1.0 - s / (2.0 * (jnp.maximum(form(left, left), 0.0) + epsilon))
            second = 1.0 - s / (2.0 * (jnp.maximum(form(right, right), 0.0) + epsilon))
            for i in left:
                fresh[i] = coef[i] * first
            for j in right:
                fresh[j] = coef[j] * second
        coef = fresh

    wide = [jnp.broadcast_to(c, (8, width)) for c in coef]

    def build(h):
        def strip(t, carry):
            rows = pl.ds(pl.multiple_of(h * block + t * 8, 8), 8)
            total = wide[0] * leaf[0, rows, :]
            for i in range(1, group):
                total = total + wide[i] * leaf[i, rows, :]
            node[h, pl.ds(pl.multiple_of(t * 8, 8), 8), :] = total
            return carry
        lax.fori_loop(0, block // 8, strip, 0)

    far = lax.rem(dp + group, n_dp)
    pieces = node_send.shape[0]
    tall = block // pieces

    def node_copy(k):
        rows = pl.ds(k * tall, tall)
        return pltpu.make_async_remote_copy(
            src_ref=node.at[1 - high, rows], dst_ref=arrived.at[rows],
            send_sem=node_send.at[k], recv_sem=node_recv.at[k],
            device_id=(far, core), device_id_type=MESH,
        )

    build(1 - high)
    for k in range(pieces):
        node_copy(k).start()
    build(high)

    sums = tuple(jnp.zeros((8, 128), jnp.float32) for _ in range(3))
    for k in range(pieces):
        node_copy(k).wait_recv()

        def inner(t, carry):
            rows = pl.ds(pl.multiple_of(k * tall + t * 8, 8), 8)
            s, q, r = carry
            for c in range(width // 128):
                a = node[high, rows, c * 128:(c + 1) * 128]
                b = arrived[rows, c * 128:(c + 1) * 128]
                s, q, r = s + a * b, q + a * a, r + b * b
            return s, q, r

        sums = lax.fori_loop(0, tall // 8, inner, sums)
    up = high.astype(jnp.float32)
    low_sq = (1.0 - up) * sums[1] + up * sums[2]
    high_sq = up * sums[1] + (1.0 - up) * sums[2]
    place = dp * 2 + core
    slots3[place] = put_lanes([sums[0], low_sq, high_sq], 8)

    def slot3_copy(q, other, at):
        return pltpu.make_async_remote_copy(
            src_ref=slots3.at[at], dst_ref=slots3.at[at],
            send_sem=slot3_send.at[q], recv_sem=slot3_recv.at[at],
            device_id=(other // 2, lax.rem(other, 2)), device_id_type=MESH,
        )

    for q in range(1, 2 * n_dp):
        slot3_copy(q, lax.rem(place + q, 2 * n_dp), place).start()
    for q in range(1, 2 * n_dp):
        other = lax.rem(place + q, 2 * n_dp)
        slot3_copy(q, other, other).wait_recv()
    line = slots3[0]
    for k in range(1, 2 * n_dp):
        line = line + slots3[k]
    line = line[0:1]
    s = lane_value(line, 0)
    low = 1.0 - s / (2.0 * (lane_value(line, 1) + epsilon))
    top = 1.0 - s / (2.0 * (lane_value(line, 2) + epsilon))
    own_coef = jnp.broadcast_to((1.0 - up) * low + up * top, (8, width))
    far_coef = jnp.broadcast_to(up * low + (1.0 - up) * top, (8, width))

    def last(t, carry):
        rows = pl.ds(pl.multiple_of(t * 8, 8), 8)
        comb[rows, :] = own_coef * node[high, rows, :] + far_coef * arrived[rows, :]
        return carry

    lax.fori_loop(0, block // 8, last, 0)

    mate_copy(0, me, core).wait_send()
    for r in range(1, group):
        i = flip(r)
        og_copy(r).wait_send()
        mate_copy(r, i, core).wait_send()
    for _, r in SLOTS:
        if r:
            for h in range(2):
                act_copy(r, flip(r), h, me).wait_send()
    part.wait_send()
    for q in range(1, 2 * group):
        slot_copy(q, lax.rem(mine + q, 2 * group), mine).wait_send()
    for k in range(pieces):
        node_copy(k).wait_send()
    for q in range(1, 2 * n_dp):
        slot3_copy(q, lax.rem(place + q, 2 * n_dp), place).wait_send()


SLOTS = ((7, 0), (5, 2), (6, 1), (4, 3))
RELAY = {1: (0, 1), 2: (0, 2), 4: (0, 4), 3: (1, 2), 6: (2, 4), 5: (4, 1), 7: (6, 1)}


def exchange(n_dp, pre_act, out_weight, out_grad):
    tokens, hidden = pre_act.shape
    block = hidden // n_dp
    group = n_dp // 2
    width = out_grad.shape[1]
    own_rows = out_grad.shape[0]
    step_cols = hidden // 8
    pieces = 4
    dma = pltpu.SemaphoreType.DMA
    hbm = pl.BlockSpec(memory_space=pl.ANY)
    vmem = pl.BlockSpec(memory_space=pltpu.VMEM)
    return pl.pallas_call(
        functools.partial(kernel, n_dp),
        out_shape=(
            jax.ShapeDtypeStruct((own_rows, width), jnp.bfloat16),
            jax.ShapeDtypeStruct((block, width), jnp.float32),
        ),
        in_specs=[hbm, hbm, hbm],
        out_specs=(vmem, vmem),
        scratch_shapes=[
            pltpu.VMEM((group, 2, tokens, block), jnp.bfloat16),
            pltpu.VMEM((group, tokens, width), jnp.bfloat16),
            pltpu.VMEM((group, 2 * block, width), jnp.float32),
            pltpu.VMEM((2, block, width), jnp.float32),
            pltpu.VMEM((block, width), jnp.float32),
            pltpu.VMEM((2, tokens, step_cols), jnp.bfloat16),
            pltpu.VMEM((2, step_cols, width), jnp.bfloat16),
            pltpu.VMEM((tokens, width), jnp.float32),
            pltpu.VMEM((own_rows, width), jnp.float32),
            pltpu.VMEM((2 * group, 8, 128), jnp.float32),
            pltpu.VMEM((2 * n_dp, 8, 128), jnp.float32),
            dma((group, 2)), dma((group, 2)), dma((group,)), dma((group,)),
            dma((group,)), dma((group,)), dma, dma((2,)),
            dma((2, 2)), dma((2,)), dma((2 * group,)), dma((2 * group,)),
            dma((pieces,)), dma((pieces,)), dma((2 * n_dp,)), dma((2 * n_dp,)),
        ],
        compiler_params=pltpu.CompilerParams(
            collective_id=0, has_side_effects=True, vmem_limit_bytes=60 * 2**20
        ),
    )(pre_act, out_weight, out_grad)


def local(pre_act, out_weight, out_grad):
    n_dp = lax.axis_size("dp")
    block = pre_act.shape[1] // n_dp
    rows = out_grad.shape[0]
    if lax.axis_size("mp") == 2 and n_dp == 4 * len(SLOTS) and block % 128 == 0 and rows % 16 == 0:
        return exchange(n_dp, pre_act, out_weight, out_grad)
    return halving(pre_act, out_weight, out_grad)


def solution(mesh):
    placed = (P("dp", "mp"), P("mp", None), P(("dp", "mp"), None))
    return jax.shard_map(
        local,
        mesh=mesh,
        in_specs=placed,
        out_specs=(P(("dp", "mp"), None), P(("mp", "dp"), None)),
        check_vma=False,
    )
```
